32 devices in a mesh: freq: 8 (over z, core), tm: 4 (over y, x).
Axes of the slice: x: 2, y: 2, z: 4, core: 2. Of those that a mesh axis runs over, the one named last changes fastest.
Arguments:
- band_state: float32 [2048, 4096], P('freq', 'tm'), may hold values from -2.5 to 2.5
- lower_rows: int32 [3, 2048], replicated, may hold values from 0 to 2047, as said below
- upper_rows: int32 [3, 2048], replicated, may hold values from 0 to 2047, as said below
- delays: int32 [3, 2048], replicated, may hold values from 0 to 1024, as said below
- counts: int32 [7], replicated, may hold values from 256 to 2048, as said below
Outputs:
- dedispersed: float32 [2048, 4096], P('freq', 'tm')
The draws below stay inside these ranges and needn't reach their ends.
Inputs may be any that keep to these rules, and one draw needn't show every extreme that they name: `counts`: entry 8 - 8 / 2^k + b is the live row count of output sub-band b of iteration k; it lies between half and all of that sub-band's 2 * 2048 / 2^(3 - k) padded rows, and in every iteration some sub-band has all its rows live. With w = 2048 / 2^(3 - k), lower_rows[k, i] is a row of input sub-band 2 * floor(i / (2 * w)) whose position in that sub-band is below its live count (all w rows are live in iteration 0). With w = 2048 / 2^(3 - k), upper_rows[k, i] is a row of input sub-band 2 * floor(i / (2 * w)) + 1 whose position in that sub-band is below its live count (all w rows are live in iteration 0). delays[k, i] is at most 2048 / 2^(3 - k), and equals it at some row in every iteration.
All inputs are finite; a program needn't handle non-finite values.
Results may differ from the reference program's by a relative error of at most 0.0003.
Values sent between devices are 32-bit elements; how exact they have to be, the bound alone decides.
A program may use at most 64 MiB of HBM per device.

```python
import jax
import jax.numpy as jnp
from jax import lax

DMAX = 2048
ITERS = 3
NT = 4096


def table_draws(key):
    count_parts = []
    lower_parts = []
    upper_parts = []
    delay_parts = []
    all_rows = jnp.arange(DMAX, dtype=jnp.int32)
    previous = jnp.full((2 ** ITERS,), DMAX >> ITERS, jnp.int32)
    for iteration in range(ITERS):
        width_in = DMAX >> ITERS - iteration
        width_out = 2 * width_in
        bands_out = DMAX // width_out
        level_keys = jax.random.split(jax.random.fold_in(key, 101 + iteration), 6)
        fresh_counts = jax.random.randint(level_keys[0], (bands_out,), width_out // 2, width_out + 1, dtype=jnp.int32)
        full_band = jax.random.randint(level_keys[5], (), 0, bands_out, dtype=jnp.int32)
        fresh_counts = jnp.where(jnp.arange(bands_out, dtype=jnp.int32) == full_band, width_out, fresh_counts)
        band_index = all_rows // width_out
        lower_live = previous[2 * band_index]
        upper_live = previous[2 * band_index + 1]
        lower_pick = jax.random.randint(level_keys[1], (DMAX,), 0, 1 << 30, dtype=jnp.int32) % lower_live
        upper_pick = jax.random.randint(level_keys[2], (DMAX,), 0, 1 << 30, dtype=jnp.int32) % upper_live
        delay_pick = jax.random.randint(level_keys[3], (DMAX,), 0, width_in + 1, dtype=jnp.int32)
        spot_row = jax.random.randint(level_keys[4], (), 0, DMAX, dtype=jnp.int32)
        delay_pick = jnp.where(all_rows == spot_row, width_in, delay_pick)
        count_parts.append(fresh_counts)
        lower_parts.append(2 * band_index * width_in + lower_pick)
        upper_parts.append((2 * band_index + 1) * width_in + upper_pick)
        delay_parts.append(delay_pick)
        previous = fresh_counts
    return (jnp.concatenate(count_parts), jnp.stack(lower_parts), jnp.stack(upper_parts), jnp.stack(delay_parts))


def draw_counts(key, part):
    return table_draws(key)[0]


def draw_lower_rows(key, part):
    return table_draws(key)[1]


def draw_upper_rows(key, part):
    return table_draws(key)[2]


def draw_delays(key, part):
    return table_draws(key)[3]


def block_levels(stream_key, dims, shards, smallest, top_value):
    def one(position, parts):
        draws = jax.random.uniform(jax.random.fold_in(jax.random.fold_in(stream_key, 6), position), (parts,), jnp.float32, smallest / len(shards), top_value / len(shards))
        return jnp.repeat(jnp.exp(draws), dims[position] // parts).reshape((-1,) + (1,) * (len(dims) - position - 1))

    loudness = one(*shards[0])
    for cut in shards[1:]:
        loudness = loudness * one(*cut)
    return loudness


def noise(key, dims, spread, limit, cuts=(), held_as=jnp.bfloat16):
    drawn = spread * jax.random.normal(key, dims, jnp.float32)
    if cuts:
        drawn = drawn * block_levels(key, dims, cuts, -0.22, 0.18)
    return jnp.clip(drawn, -limit, limit).astype(held_as)


def setup_inputs(seed: int = 0) -> dict:
    streams_of = jax.random.split(jax.random.key(seed), 6)
    band_state = noise(streams_of[0], (DMAX, NT), 0.35, 2.5, ((0, 8), (1, 4)), jnp.float32)
    lower_rows = draw_lower_rows(jax.random.fold_in(streams_of[5], 71), 0)
    upper_rows = draw_upper_rows(jax.random.fold_in(streams_of[5], 71), 0)
    delays = draw_delays(jax.random.fold_in(streams_of[5], 71), 0)
    counts = draw_counts(jax.random.fold_in(streams_of[5], 71), 0)
    return {"band_state": band_state, "lower_rows": lower_rows, "upper_rows": upper_rows, "delays": delays, "counts": counts}


def delayed_rows(source_rows, shifts):
    positions = jnp.arange(source_rows.shape[1], dtype=jnp.int32)[None, :] - shifts[:, None]
    picked = jnp.take_along_axis(source_rows, jnp.maximum(positions, 0), axis=1)
    return jnp.where(positions >= 0, picked, jnp.zeros_like(picked))


def reference(band_state, lower_rows, upper_rows, delays, counts):
    block_rows = min(DMAX, 512)
    all_rows = jnp.arange(DMAX, dtype=jnp.int32)
    current = band_state
    for iteration in range(ITERS):
        width_out = DMAX >> (ITERS - iteration - 1)
        offset = 2 ** ITERS - 2 ** (ITERS - iteration)
        live_rows = (all_rows % width_out) < counts[offset + all_rows // width_out]

        def merge_block(pieces, current=current):
            lower_index, upper_index, shifts, keep_rows = pieces
            summed = current[lower_index] + delayed_rows(current[upper_index], shifts)
            return jnp.where(keep_rows[:, None], summed, jnp.zeros_like(summed))

        pieces = (lower_rows[iteration].reshape(-1, block_rows),
                  upper_rows[iteration].reshape(-1, block_rows),
                  delays[iteration].reshape(-1, block_rows),
                  live_rows.reshape(-1, block_rows))
        merged = lax.map(merge_block, pieces)
        current = merged.reshape(DMAX, -1)
    return current
```

```python
import functools

import jax
import jax.numpy as jnp
from jax import lax
from jax.experimental import pallas as pl
from jax.experimental.pallas import tpu as pltpu
from jax.sharding import PartitionSpec as P

DMAX = 2048
ITERS = 3
LANES = 128
UNROLL = 8
CHUNKS_1 = 8
CHUNKS_2 = 16


def shifted_2(block, axis, distance):
    devices = range(lax.axis_size(axis))
    route = [(i - distance, i) for i in devices if i - distance in devices]
    return lax.ppermute(block, axis, route)


def delay_columns(extended, shifts, widest):
    row_count = extended.shape[0]
    for bit_index in range(widest.bit_length()):
        stride = 1 << bit_index
        shifted = jnp.concatenate(
            [jnp.zeros((row_count, stride), extended.dtype), extended[:, :-stride]], axis=1
        )
        extended = jnp.where((shifts >> bit_index & 1)[:, None] == 1, shifted, extended)
    return extended


def live_mask(global_rows, counts, width_out, offset, bands_out):
    band_index = global_rows // width_out
    band_counts = counts[offset : offset + bands_out]
    matches = band_index[:, None] == jnp.arange(bands_out, dtype=jnp.int32)[None, :]
    live_count = jnp.sum(jnp.where(matches, band_counts[None, :], 0), axis=1)
    return global_rows % width_out < live_count


def per_device_general(band_state, lower_rows, upper_rows, delays, counts):
    row_count, samples = band_state.shape
    freq_index = lax.axis_index("freq")
    first_row = freq_index * row_count
    global_rows = first_row + jnp.arange(row_count, dtype=jnp.int32)
    current = band_state
    for iteration in range(ITERS):
        width_in = DMAX >> ITERS - iteration
        width_out = 2 * width_in
        bands_out = DMAX // width_out
        offset = 2**ITERS - 2 ** (ITERS - iteration)
        lower_source = lax.dynamic_slice_in_dim(lower_rows[iteration], first_row, row_count)
        upper_source = lax.dynamic_slice_in_dim(upper_rows[iteration], first_row, row_count)
        own_delays = lax.dynamic_slice_in_dim(delays[iteration], first_row, row_count)
        gathered = lax.all_gather(current, "freq", axis=0, tiled=True)
        lower_values = jnp.take(gathered, lower_source, axis=0)
        upper_values = jnp.take(gathered, upper_source, axis=0)
        rim_columns = shifted_2(upper_values[:, samples - width_in :], "tm", 1)
        extended = jnp.concatenate([rim_columns, upper_values], axis=1)
        delayed = delay_columns(extended, own_delays, width_in)[:, width_in:]
        live_rows = live_mask(global_rows, counts, width_out, offset, bands_out)
        current = jnp.where(live_rows[:, None], lower_values + delayed, jnp.zeros_like(delayed))
    return current


class Flow:
    def __init__(self, buffer, sems, first, chunk):
        self.buffer, self.sems, self.first, self.chunk = buffer, sems, first, chunk

    def copy(self, j, row, target, source_at, target_at, size):
        rows = pl.ds(row + j * self.chunk, self.chunk)
        return pltpu.make_async_remote_copy(
            src_ref=self.buffer.at[rows, pl.ds(source_at, size)],
            dst_ref=self.buffer.at[rows, pl.ds(target_at, size)],
            send_sem=self.sems.at[0, self.first + j],
            recv_sem=self.sems.at[1, self.first + j],
            device_id=target,
            device_id_type=pl.DeviceIdType.MESH,
        )


def kernel(tiles, tm_size, x_ref, lower, upper, delays, counts, out_ref, b0, b1, b2, s0, s1, s2, local_sem):
    f, t = lax.axis_index("freq"), lax.axis_index("tm")
    c, z = lax.rem(f, 2), lax.div(f, 2)
    zb, half = lax.rem(z, 2), lax.div(z, 2)
    z_size = 2 ** (ITERS - 1)
    rows = x_ref.shape[0]
    at = lambda ff, tt: {"freq": ff, "tm": tt}
    partner = at(f + 1 - 2 * c, t)
    later = at(f, t + 1)
    pair = at(f + 2 - 4 * zb, t)
    inner = zb != half
    facing = at(f + 2 - 4 * half, t)
    outer = at(f - 2 + 4 * half, t)
    has_later, has_earlier = t < tm_size - 1, t > 0

    barrier = pltpu.get_barrier_semaphore()

    def greet(target):
        pl.semaphore_signal(barrier, inc=1, device_id=target, device_id_type=pl.DeviceIdType.MESH)

    greet(partner)
    for cond, target in (
        (z > 0, at(f - 2, t)),
        (z < z_size - 1, at(f + 2, t)),
        (has_earlier, at(f, t - 1)),
        (has_later, later),
    ):
        pl.when(cond)(functools.partial(greet, target))
    one = lambda cond: jnp.where(cond, 1, 0)
    pl.semaphore_wait(barrier, 1 + one(z > 0) + one(z < z_size - 1) + one(has_earlier) + one(has_later))

    lane = lax.broadcasted_iota(jnp.int32, (tiles, LANES), 1)

    def merge(k, source, first, position, start, count, store):
        width_in = DMAX >> ITERS - k
        rim = width_in // LANES
        width_out = 2 * width_in
        band = lax.div(first, width_out)
        limit = counts[2**ITERS - 2 ** (ITERS - k) + band]
        wrap = width_out - 1

        def body(step, carry):
            values = []
            for u in range(UNROLL):
                i = start + step * UNROLL + u
                g = first + i
                lo, up, d = lower[k, g] & wrap, upper[k, g] & wrap, delays[k, g]
                q, r = d >> 7, d & (LANES - 1)
                a = source[up, pl.ds(tiles - q, tiles), :]
                b = source[up, pl.ds(jnp.maximum(tiles - 1 - q, tiles - rim), tiles), :]
                a, b = pltpu.roll(a, r, 1), pltpu.roll(b, r, 1)
                total = source[lo, tiles:, :] + jnp.where(lane >= r, a, b)
                values.append((i, jnp.where(position + i < limit, total, jnp.zeros_like(total))))
            for i, value in values:
                store(i, value)
            return carry

        lax.fori_loop(0, count // UNROLL, body, 0)

    def when(cond, action):
        pl.when(cond)(action)

    rim0 = rows // LANES
    own0 = Flow(b0, s0, 0, rows)
    rim_out0 = Flow(b0, s0, 1, rows)
    rim_in0 = Flow(b0, s0, 2, rows)
    stage = pltpu.make_async_copy(x_ref, b0.at[pl.ds(c * rows, rows), pl.ds(tiles, tiles)], local_sem.at[0])
    stage.start()
    stage.wait()
    own0.copy(0, c * rows, partner, tiles, tiles, tiles).start()
    upper0 = rows
    send_rim0 = rim_out0.copy(0, upper0, later, 2 * tiles - rim0, tiles - rim0, rim0)
    pass_rim0 = rim_in0.copy(0, upper0, partner, tiles - rim0, tiles - rim0, rim0)
    when((c == 1) & has_later, send_rim0.start)

    @pl.when(t == 0)
    def _():
        for buffer in (b0, b1, b2):
            first = buffer.shape[0] // 2

            def clear(i, carry, buffer=buffer, first=first):
                for u in range(UNROLL):
                    buffer[first + i * UNROLL + u, :tiles, :] = jnp.zeros((tiles, LANES), jnp.float32)
                return carry

            lax.fori_loop(0, first // UNROLL, clear, 0)

    @pl.when((c == 1) & has_earlier)
    def _():
        send_rim0.wait_recv()
        pass_rim0.start()

    own0.copy(0, (1 - c) * rows, partner, tiles, tiles, tiles).wait_recv()
    when((c == 0) & has_earlier, pass_rim0.wait_recv)

    rim1 = 2 * rows // LANES
    n1, chunk1 = CHUNKS_1, rows // CHUNKS_1
    flows1 = [Flow(b1, s1, kind * n1, chunk1) for kind in range(5)]
    own1, pair1, pass1, rim_out1, rim_in1 = flows1
    mine1 = zb * 2 * rows + c * rows
    other1 = (1 - zb) * 2 * rows + c * rows
    upper1 = 2 * rows + c * rows
    wide = (tiles, tiles, tiles)
    tail1 = (2 * tiles - rim1, tiles - rim1, rim1)
    kept1 = (tiles - rim1, tiles - rim1, rim1)

    def store1(i, value):
        b1[mine1 + i, tiles:, :] = value

    for j in range(n1):
        merge(0, b0, f * rows, c * rows, j * chunk1, chunk1, store1)
        pair1.copy(j, mine1, pair, *wide).start()
        own1.copy(j, mine1, partner, *wide).start()
        when((zb == 1) & has_later, rim_out1.copy(j, upper1, later, *tail1).start)
    for j in range(n1):
        pair1.copy(j, other1, pair, *wide).wait_recv()
        when((zb == 0) & has_later, rim_out1.copy(j, upper1, later, *tail1).start)
        pass1.copy(j, other1, partner, *wide).start()

        @pl.when(has_earlier)
        def _():
            rim_out1.copy(j, upper1, later, *tail1).wait_recv()
            rim_in1.copy(j, upper1, partner, *kept1).start()

    across = (1 - 2 * c) * rows
    for j in range(n1):
        own1.copy(j, mine1 + across, partner, *wide).wait_recv()
        pass1.copy(j, other1 + across, partner, *wide).wait_recv()
        when(has_earlier, rim_in1.copy(j, upper1 + across, partner, *kept1).wait_recv)

    n2, chunk2 = CHUNKS_2, 2 * rows // CHUNKS_2
    flows2 = [Flow(b2, s2, kind * n2, chunk2) for kind in range(5)]
    own2, z2, pass2, rim_out2, rim_in2 = flows2
    mine2 = half * 4 * rows + c * 2 * rows
    other2 = (1 - half) * 4 * rows + c * 2 * rows
    upper2 = 4 * rows + c * 2 * rows
    tail2 = (tiles, 0, tiles)
    kept2 = (0, 0, tiles)

    def store2(i, value):
        b2[mine2 + i, tiles:, :] = value

    for j in range(n2):
        merge(1, b1, half * 4 * rows + c * 2 * rows, c * 2 * rows, j * chunk2, chunk2, store2)
        when(inner, z2.copy(j, mine2, facing, *wide).start)
        when((half == 1) & has_later, rim_out2.copy(j, upper2, later, *tail2).start)
        own2.copy(j, mine2, partner, *wide).start()
    for j in range(n2):
        z2.copy(j, other2, partner, *wide).wait_recv()
        when(
            inner,
            pltpu.make_async_remote_copy(
                src_ref=b2.at[pl.ds(other2 + j * chunk2, chunk2), pl.ds(tiles, tiles)],
                dst_ref=b2.at[pl.ds(other2 + j * chunk2, chunk2), pl.ds(tiles, tiles)],
                send_sem=s2.at[0, 5 * n2 + j],
                recv_sem=s2.at[1, n2 + j],
                device_id=outer,
                device_id_type=pl.DeviceIdType.MESH,
            ).start,
        )
        when((half == 0) & has_later, rim_out2.copy(j, upper2, later, *tail2).start)
        pass2.copy(j, other2, partner, *wide).start()

        @pl.when(has_earlier)
        def _():
            rim_out2.copy(j, upper2, later, *tail2).wait_recv()
            rim_in2.copy(j, upper2, partner, *kept2).start()

    across = (1 - 2 * c) * 2 * rows
    for j in range(n2):
        own2.copy(j, mine2 + across, partner, *wide).wait_recv()
        pass2.copy(j, other2 + across, partner, *wide).wait_recv()
        when(has_earlier, rim_in2.copy(j, upper2 + across, partner, *kept2).wait_recv)

    def store_out(i, value):
        out_ref[i] = value

    merge(2, b2, f * rows, f * rows, 0, rows, store_out)

    own0.copy(0, c * rows, partner, *wide).wait_send()
    when((c == 1) & has_later, send_rim0.wait_send)
    when((c == 1) & has_earlier, pass_rim0.wait_send)
    for j in range(n1):
        pair1.copy(j, mine1, pair, *wide).wait_send()
        own1.copy(j, mine1, partner, *wide).wait_send()
        pass1.copy(j, other1, partner, *wide).wait_send()
        when(has_later, rim_out1.copy(j, upper1, later, *tail1).wait_send)
        when(has_earlier, rim_in1.copy(j, upper1, partner, *kept1).wait_send)
    for j in range(n2):
        own2.copy(j, mine2, partner, *wide).wait_send()
        pass2.copy(j, other2, partner, *wide).wait_send()
        when(has_later, rim_out2.copy(j, upper2, later, *tail2).wait_send)
        when(has_earlier, rim_in2.copy(j, upper2, partner, *kept2).wait_send)

        @pl.when(inner)
        def _():
            z2.copy(j, mine2, facing, *wide).wait_send()
            pltpu.make_async_remote_copy(
                src_ref=b2.at[pl.ds(other2 + j * chunk2, chunk2), pl.ds(tiles, tiles)],
                dst_ref=b2.at[pl.ds(other2 + j * chunk2, chunk2), pl.ds(tiles, tiles)],
                send_sem=s2.at[0, 5 * n2 + j],
                recv_sem=s2.at[1, n2 + j],
                device_id=outer,
                device_id_type=pl.DeviceIdType.MESH,
            ).wait_send()


def per_device_fused(tm_size, band_state, lower_rows, upper_rows, delays, counts):
    row_count, samples = band_state.shape
    tiles = samples // LANES
    dma = pltpu.SemaphoreType.DMA
    out = pl.pallas_call(
        functools.partial(kernel, tiles, tm_size),
        out_shape=jax.ShapeDtypeStruct((row_count, tiles, LANES), jnp.float32),
        in_specs=[pl.BlockSpec(memory_space=pltpu.VMEM)] + [pl.BlockSpec(memory_space=pltpu.SMEM)] * 4,
        out_specs=pl.BlockSpec(memory_space=pltpu.VMEM),
        scratch_shapes=[
            pltpu.VMEM((2 * row_count, 2 * tiles, LANES), jnp.float32),
            pltpu.VMEM((4 * row_count, 2 * tiles, LANES), jnp.float32),
            pltpu.VMEM((8 * row_count, 2 * tiles, LANES), jnp.float32),
            dma((2, 3)),
            dma((2, 5 * CHUNKS_1)),
            dma((2, 6 * CHUNKS_2)),
            dma((1,)),
        ],
        compiler_params=pltpu.CompilerParams(
            collective_id=0, has_side_effects=True, vmem_limit_bytes=60 * 2**20
        ),
    )(band_state.reshape(row_count, tiles, LANES), lower_rows, upper_rows, delays, counts)
    return out.reshape(row_count, samples)


def solution(mesh):
    if mesh.shape["freq"] == 2**ITERS:
        body = functools.partial(per_device_fused, mesh.shape["tm"])
    else:
        body = per_device_general
    return jax.shard_map(
        body,
        mesh=mesh,
        in_specs=(P("freq", "tm"), P(), P(), P(), P()),
        out_specs=P("freq", "tm"),
        check_vma=False,
    )
```

```python
import functools

import jax
import jax.numpy as jnp
from jax import lax
from jax.experimental import pallas as pl
from jax.experimental.pallas import tpu as pltpu
from jax.sharding import PartitionSpec as P

DMAX = 2048
ITERS = 3
LANES = 128
SUBLANES = 8
UNROLL = 16
CHUNKS_0 = 4
CHUNKS_1 = 8
CHUNKS_2 = 16


def shifted_2(block, axis, distance):
    devices = range(lax.axis_size(axis))
    route = [(i - distance, i) for i in devices if i - distance in devices]
    return lax.ppermute(block, axis, route)


def delay_columns(extended, shifts, widest):
    row_count = extended.shape[0]
    for bit_index in range(widest.bit_length()):
        stride = 1 << bit_index
        shifted = jnp.concatenate(
            [jnp.zeros((row_count, stride), extended.dtype), extended[:, :-stride]], axis=1
        )
        extended = jnp.where((shifts >> bit_index & 1)[:, None] == 1, shifted, extended)
    return extended


def live_mask(global_rows, counts, width_out, offset, bands_out):
    band_index = global_rows // width_out
    band_counts = counts[offset : offset + bands_out]
    matches = band_index[:, None] == jnp.arange(bands_out, dtype=jnp.int32)[None, :]
    live_count = jnp.sum(jnp.where(matches, band_counts[None, :], 0), axis=1)
    return global_rows % width_out < live_count


def per_device_general(band_state, lower_rows, upper_rows, delays, counts):
    row_count, samples = band_state.shape
    freq_index = lax.axis_index("freq")
    first_row = freq_index * row_count
    global_rows = first_row + jnp.arange(row_count, dtype=jnp.int32)
    current = band_state
    for iteration in range(ITERS):
        width_in = DMAX >> ITERS - iteration
        width_out = 2 * width_in
        bands_out = DMAX // width_out
        offset = 2**ITERS - 2 ** (ITERS - iteration)
        lower_source = lax.dynamic_slice_in_dim(lower_rows[iteration], first_row, row_count)
        upper_source = lax.dynamic_slice_in_dim(upper_rows[iteration], first_row, row_count)
        own_delays = lax.dynamic_slice_in_dim(delays[iteration], first_row, row_count)
        gathered = lax.all_gather(current, "freq", axis=0, tiled=True)
        lower_values = jnp.take(gathered, lower_source, axis=0)
        upper_values = jnp.take(gathered, upper_source, axis=0)
        rim_columns = shifted_2(upper_values[:, samples - width_in :], "tm", 1)
        extended = jnp.concatenate([rim_columns, upper_values], axis=1)
        delayed = delay_columns(extended, own_delays, width_in)[:, width_in:]
        live_rows = live_mask(global_rows, counts, width_out, offset, bands_out)
        current = jnp.where(live_rows[:, None], lower_values + delayed, jnp.zeros_like(delayed))
    return current


class Flow:
    def __init__(self, buffer, sems, first, chunk):
        self.buffer, self.sems, self.first, self.chunk = buffer, sems, first, chunk

    def copy(self, j, row, target, source_at, target_at, size):
        rows = pl.ds(row + j * self.chunk, self.chunk)
        return pltpu.make_async_remote_copy(
            src_ref=self.buffer.at[rows, pl.ds(source_at, size)],
            dst_ref=self.buffer.at[rows, pl.ds(target_at, size)],
            send_sem=self.sems.at[0, self.first + j],
            recv_sem=self.sems.at[1, self.first + j],
            device_id=target,
            device_id_type=pl.DeviceIdType.MESH,
        )


def kernel(tiles, tm_size, x_ref, lower, upper, delays, counts, out_ref, b0, b1, b2, final, s0, s1, s2):
    f, t = lax.axis_index("freq"), lax.axis_index("tm")
    c, z = lax.rem(f, 2), lax.div(f, 2)
    zb, half = lax.rem(z, 2), lax.div(z, 2)
    z_size = 2 ** (ITERS - 1)
    rows = x_ref.shape[0]
    at = lambda ff, tt: {"freq": ff, "tm": tt}
    partner = at(f + 1 - 2 * c, t)
    later = at(f, t + 1)
    pair = at(f + 2 - 4 * zb, t)
    inner = zb != half
    facing = at(f + 2 - 4 * half, t)
    outer = at(f - 2 + 4 * half, t)
    has_later, has_earlier = t < tm_size - 1, t > 0

    barrier = pltpu.get_barrier_semaphore()

    def greet(target):
        pl.semaphore_signal(barrier, inc=1, device_id=target, device_id_type=pl.DeviceIdType.MESH)

    greet(partner)
    for cond, target in (
        (z > 0, at(f - 2, t)),
        (z < z_size - 1, at(f + 2, t)),
        (has_earlier, at(f, t - 1)),
        (has_later, later),
    ):
        pl.when(cond)(functools.partial(greet, target))
    one = lambda cond: jnp.where(cond, 1, 0)
    pl.semaphore_wait(barrier, 1 + one(z > 0) + one(z < z_size - 1) + one(has_earlier) + one(has_later))

    lane = lax.broadcasted_iota(jnp.int32, (tiles, LANES), 1)

    def merge(k, source, first, position, start, count, store):
        width_in = DMAX >> ITERS - k
        rim = width_in // LANES
        width_out = 2 * width_in
        band = lax.div(first, width_out)
        limit = counts[2**ITERS - 2 ** (ITERS - k) + band]
        wrap = width_out - 1

        def body(step, carry):
            values = []
            for u in range(UNROLL):
                i = start + step * UNROLL + u
                g = first + i
                lo, up, d = lower[k, g] & wrap, upper[k, g] & wrap, delays[k, g]
                q, r = d >> 7, d & (LANES - 1)
                a = source[up, pl.ds(tiles - q, tiles), :]
                b = source[up, pl.ds(jnp.maximum(tiles - 1 - q, tiles - rim), tiles), :]
                a, b = pltpu.roll(a, r, 1), pltpu.roll(b, r, 1)
                total = source[lo, tiles:, :] + jnp.where(lane >= r, a, b)
                values.append((i, jnp.where(position + i < limit, total, jnp.zeros_like(total))))
            for i, value in values:
                store(i, value)
            return carry

        lax.fori_loop(0, count // UNROLL, body, 0)

    def when(cond, action):
        pl.when(cond)(action)

    rim0 = rows // LANES
    n0, chunk0 = CHUNKS_0, rows // CHUNKS_0
    own0, rim_out0, rim_in0 = [Flow(b0, s0, kind * n0, chunk0) for kind in range(3)]
    upper0 = rows
    tail0 = (2 * tiles - rim0, tiles - rim0, rim0)
    kept0 = (tiles - rim0, tiles - rim0, rim0)
    full0 = (tiles, tiles, tiles)

    def spread(first, count):
        def body(step, carry):
            r = first + step * SUBLANES
            for tile in range(tiles):
                b0[pl.ds(c * rows + r, SUBLANES), tiles + tile, :] = x_ref[
                    pl.ds(r, SUBLANES), pl.ds(tile * LANES, LANES)
                ]
            return carry

        lax.fori_loop(0, count // SUBLANES, body, 0)

    for j in range(n0):
        spread(j * chunk0, chunk0)
        when((c == 1) & has_later, rim_out0.copy(j, upper0, later, *tail0).start)
        own0.copy(j, c * rows, partner, *full0).start()

    @pl.when(t == 0)
    def _():
        for buffer in (b0, b1, b2):
            first = buffer.shape[0] // 2

            def clear(i, carry, buffer=buffer, first=first):
                for u in range(UNROLL):
                    buffer[first + i * UNROLL + u, :tiles, :] = jnp.zeros((tiles, LANES), jnp.float32)
                return carry

            lax.fori_loop(0, first // UNROLL, clear, 0)

    for j in range(n0):

        @pl.when((c == 1) & has_earlier)
        def _():
            rim_out0.copy(j, upper0, later, *tail0).wait_recv()
            rim_in0.copy(j, upper0, partner, *kept0).start()

    for j in range(n0):
        own0.copy(j, (1 - c) * rows, partner, *full0).wait_recv()
        when((c == 0) & has_earlier, rim_in0.copy(j, upper0, partner, *kept0).wait_recv)

    rim1 = 2 * rows // LANES
    n1, chunk1 = CHUNKS_1, rows // CHUNKS_1
    flows1 = [Flow(b1, s1, kind * n1, chunk1) for kind in range(5)]
    own1, pair1, pass1, rim_out1, rim_in1 = flows1
    mine1 = zb * 2 * rows + c * rows
    other1 = (1 - zb) * 2 * rows + c * rows
    upper1 = 2 * rows + c * rows
    wide = (tiles, tiles, tiles)
    tail1 = (2 * tiles - rim1, tiles - rim1, rim1)
    kept1 = (tiles - rim1, tiles - rim1, rim1)

    def store1(i, value):
        b1[mine1 + i, tiles:, :] = value

    for j in range(n1):
        merge(0, b0, f * rows, c * rows, j * chunk1, chunk1, store1)
        pair1.copy(j, mine1, pair, *wide).start()
        own1.copy(j, mine1, partner, *wide).start()
        when((zb == 1) & has_later, rim_out1.copy(j, upper1, later, *tail1).start)
    for j in range(n1):
        pair1.copy(j, other1, pair, *wide).wait_recv()
        when((zb == 0) & has_later, rim_out1.copy(j, upper1, later, *tail1).start)
        pass1.copy(j, other1, partner, *wide).start()

        @pl.when(has_earlier)
        def _():
            rim_out1.copy(j, upper1, later, *tail1).wait_recv()
            rim_in1.copy(j, upper1, partner, *kept1).start()

    across = (1 - 2 * c) * rows
    for j in range(n1):
        own1.copy(j, mine1 + across, partner, *wide).wait_recv()
        pass1.copy(j, other1 + across, partner, *wide).wait_recv()
        when(has_earlier, rim_in1.copy(j, upper1 + across, partner, *kept1).wait_recv)

    n2, chunk2 = CHUNKS_2, 2 * rows // CHUNKS_2
    flows2 = [Flow(b2, s2, kind * n2, chunk2) for kind in range(5)]
    own2, z2, pass2, rim_out2, rim_in2 = flows2
    mine2 = half * 4 * rows + c * 2 * rows
    other2 = (1 - half) * 4 * rows + c * 2 * rows
    upper2 = 4 * rows + c * 2 * rows
    tail2 = (tiles, 0, tiles)
    kept2 = (0, 0, tiles)

    def store2(i, value):
        b2[mine2 + i, tiles:, :] = value

    for j in range(n2):
        merge(1, b1, half * 4 * rows + c * 2 * rows, c * 2 * rows, j * chunk2, chunk2, store2)
        when(inner, z2.copy(j, mine2, facing, *wide).start)
        when((half == 1) & has_later, rim_out2.copy(j, upper2, later, *tail2).start)
        own2.copy(j, mine2, partner, *wide).start()
    for j in range(n2):
        z2.copy(j, other2, partner, *wide).wait_recv()
        when(
            inner,
            pltpu.make_async_remote_copy(
                src_ref=b2.at[pl.ds(other2 + j * chunk2, chunk2), pl.ds(tiles, tiles)],
                dst_ref=b2.at[pl.ds(other2 + j * chunk2, chunk2), pl.ds(tiles, tiles)],
                send_sem=s2.at[0, 5 * n2 + j],
                recv_sem=s2.at[1, n2 + j],
                device_id=outer,
                device_id_type=pl.DeviceIdType.MESH,
            ).start,
        )
        when((half == 0) & has_later, rim_out2.copy(j, upper2, later, *tail2).start)
        pass2.copy(j, other2, partner, *wide).start()

        @pl.when(has_earlier)
        def _():
            rim_out2.copy(j, upper2, later, *tail2).wait_recv()
            rim_in2.copy(j, upper2, partner, *kept2).start()

    across = (1 - 2 * c) * 2 * rows
    for j in range(n2):
        own2.copy(j, mine2 + across, partner, *wide).wait_recv()
        pass2.copy(j, other2 + across, partner, *wide).wait_recv()
        when(has_earlier, rim_in2.copy(j, upper2 + across, partner, *kept2).wait_recv)

    def store_out(i, value):
        final[i] = value

    merge(2, b2, f * rows, f * rows, 0, rows, store_out)

    def flatten(step, carry):
        r = step * SUBLANES
        for tile in range(tiles):
            out_ref[pl.ds(r, SUBLANES), pl.ds(tile * LANES, LANES)] = final[pl.ds(r, SUBLANES), tile, :]
        return carry

    lax.fori_loop(0, rows // SUBLANES, flatten, 0)

    for j in range(n0):
        own0.copy(j, c * rows, partner, *full0).wait_send()
        when((c == 1) & has_later, rim_out0.copy(j, upper0, later, *tail0).wait_send)
        when((c == 1) & has_earlier, rim_in0.copy(j, upper0, partner, *kept0).wait_send)
    for j in range(n1):
        pair1.copy(j, mine1, pair, *wide).wait_send()
        own1.copy(j, mine1, partner, *wide).wait_send()
        pass1.copy(j, other1, partner, *wide).wait_send()
        when(has_later, rim_out1.copy(j, upper1, later, *tail1).wait_send)
        when(has_earlier, rim_in1.copy(j, upper1, partner, *kept1).wait_send)
    for j in range(n2):
        own2.copy(j, mine2, partner, *wide).wait_send()
        pass2.copy(j, other2, partner, *wide).wait_send()
        when(has_later, rim_out2.copy(j, upper2, later, *tail2).wait_send)
        when(has_earlier, rim_in2.copy(j, upper2, partner, *kept2).wait_send)

        @pl.when(inner)
        def _():
            z2.copy(j, mine2, facing, *wide).wait_send()
            pltpu.make_async_remote_copy(
                src_ref=b2.at[pl.ds(other2 + j * chunk2, chunk2), pl.ds(tiles, tiles)],
                dst_ref=b2.at[pl.ds(other2 + j * chunk2, chunk2), pl.ds(tiles, tiles)],
                send_sem=s2.at[0, 5 * n2 + j],
                recv_sem=s2.at[1, n2 + j],
                device_id=outer,
                device_id_type=pl.DeviceIdType.MESH,
            ).wait_send()


def per_device_fused(tm_size, band_state, lower_rows, upper_rows, delays, counts):
    row_count, samples = band_state.shape
    tiles = samples // LANES
    dma = pltpu.SemaphoreType.DMA
    return pl.pallas_call(
        functools.partial(kernel, tiles, tm_size),
        out_shape=jax.ShapeDtypeStruct((row_count, samples), jnp.float32),
        in_specs=[pl.BlockSpec(memory_space=pltpu.VMEM)] + [pl.BlockSpec(memory_space=pltpu.SMEM)] * 4,
        out_specs=pl.BlockSpec(memory_space=pltpu.VMEM),
        scratch_shapes=[
            pltpu.VMEM((2 * row_count, 2 * tiles, LANES), jnp.float32),
            pltpu.VMEM((4 * row_count, 2 * tiles, LANES), jnp.float32),
            pltpu.VMEM((8 * row_count, 2 * tiles, LANES), jnp.float32),
            pltpu.VMEM((row_count, tiles, LANES), jnp.float32),
            dma((2, 3 * CHUNKS_0)),
            dma((2, 5 * CHUNKS_1)),
            dma((2, 6 * CHUNKS_2)),
        ],
        compiler_params=pltpu.CompilerParams(
            collective_id=0, has_side_effects=True, vmem_limit_bytes=60 * 2**20
        ),
    )(band_state, lower_rows, upper_rows, delays, counts)


def solution(mesh):
    if mesh.shape["freq"] == 2**ITERS:
        body = functools.partial(per_device_fused, mesh.shape["tm"])
    else:
        body = per_device_general
    return jax.shard_map(
        body,
        mesh=mesh,
        in_specs=(P("freq", "tm"), P(), P(), P(), P()),
        out_specs=P("freq", "tm"),
        check_vma=False,
    )
```
